256 devices in a mesh: gx: 16 (over y_lo, x, core), gy: 16 (over z, y_hi).
Axes of the slice: x: 4, y: 4 (y_hi: 2, y_lo: 2; y = y_hi * 2 + y_lo), z: 8, core: 2. Of those that a mesh axis runs over, the one named last changes fastest.
Arguments:
- east_class: int32 [1024, 1024], P('gx', 'gy'), may hold values from 0 to 7
- south_class: int32 [1024, 1024], P('gx', 'gy'), may hold values from 0 to 7
- cond_table: float32 [8], replicated, may hold values from 0.5 to 4
- leakage: float32 [1024, 1024], P('gx', 'gy'), may hold values from 0.1 to 1
- pad_mask: int32 [1024, 1024], P('gx', 'gy'), may hold values 0 or 1
- load_current: float32 [1024, 1024, 256], P('gx', 'gy'), may hold values from -24 to 24
Outputs:
- potential: float32 [1024, 1024, 256], P('gx', 'gy')
The draws below stay inside these ranges and needn't reach their ends.
All inputs are finite; a program needn't handle non-finite values. No bound on the sum of `pad_mask` on one device may be relied on, other than what follows from the above.
Results may differ from the reference program's by a relative error of at most 0.00002.
Values sent between devices are 32-bit elements; how exact they have to be, the bound alone decides.
A program may use at most 64 MiB of HBM per device.

```python
import math
import jax
import jax.numpy as jnp

CASES = 256
CLASSES = 8
ITERS = 4
NX = 1024
NY = 1024


def touch_ends(values, key, smallest, top_value):
    extent = values.shape
    spot = [jax.random.randint(jax.random.fold_in(key, axis), (), 0, extent[axis]) for axis in range(len(extent))]
    values = values.at[tuple(spot)].set(smallest)
    longest = extent.index(max(extent))
    spot[longest] = (spot[longest] + 1) % extent[longest]
    return values.at[tuple(spot)].set(top_value)


def shard_levels(stream_key, shape, pieces, smallest, high):
    gain, own = 1.0, jax.random.fold_in(stream_key, 6)
    for axis_at, shards_of in pieces:
        draws = jnp.exp(jax.random.uniform(jax.random.fold_in(own, axis_at), (shards_of,), jnp.float32, smallest / len(pieces), high / len(pieces)))
        gain = gain * jnp.repeat(draws, shape[axis_at] // shards_of).reshape([-1 if axis == axis_at else 1 for axis in range(len(shape))])
    return gain


def scatter_about(stream_key, dims, deviation, bound, split=(), kind=jnp.bfloat16):
    array = deviation * jax.random.normal(stream_key, dims, jnp.float32)
    if split:
        array = array * shard_levels(stream_key, dims, split, -0.22, 0.18)
    return jnp.clip(array, -bound, bound).astype(kind)


def setup_inputs(seed: int = 0) -> dict:
    streams_of = jax.random.split(jax.random.key(seed), 7)
    east_class = touch_ends(jax.random.randint(streams_of[0], (NX, NY), 0, CLASSES), jax.random.fold_in(streams_of[0], 1), 0, CLASSES - 1).astype(jnp.int32)
    south_class = touch_ends(jax.random.randint(streams_of[1], (NX, NY), 0, CLASSES), jax.random.fold_in(streams_of[1], 1), 0, CLASSES - 1).astype(jnp.int32)
    cond_table = jnp.clip(jnp.exp(jax.random.uniform(streams_of[2], (CLASSES,), jnp.float32, math.log(0.5), math.log(4.0))), 0.5, 4.0)
    leakage = jnp.clip(jnp.exp(math.log(1.0) - 2.3025851 * jax.random.uniform(streams_of[3], (NX, NY), jnp.float32) ** shard_levels(streams_of[3], (NX, NY), ((0, 16), (1, 16)), -0.2, 0.2)), 0.1, 1.0)
    pad_mask = touch_ends((jax.random.randint(streams_of[4], (NX, NY), 0, 8) < 1).astype(jnp.int32), jax.random.fold_in(streams_of[4], 1), 0, 1)
    load_current = scatter_about(streams_of[5], (NX, NY, CASES), 4.0, 24.0, ((0, 16), (1, 16)), jnp.float32)
    return dict(east_class=east_class, south_class=south_class, cond_table=cond_table, leakage=leakage, pad_mask=pad_mask, load_current=load_current)


PAD_GAIN = 8.0
SPECTRAL_BOUND = 0.995


def chebyshev_weights(total_steps):
    weights = [1.0]
    for position in range(1, total_steps):
        if position == 1:
            weights.append(1.0 / (1.0 - SPECTRAL_BOUND * SPECTRAL_BOUND / 2.0))
        else:
            weights.append(1.0 / (1.0 - SPECTRAL_BOUND * SPECTRAL_BOUND * weights[-1] / 4.0))
    return weights


def lookup(classes, cond_table):
    labels = jnp.arange(cond_table.shape[0], dtype=jnp.int32)
    matches = classes[:, :, None] == labels
    return jnp.sum(jnp.where(matches, cond_table, 0.0), axis=-1)


def reference(east_class, south_class, cond_table, leakage, pad_mask, load_current):
    east_cond = lookup(east_class, cond_table)
    south_cond = lookup(south_class, cond_table)
    pads = pad_mask.astype(jnp.float32)
    east_west = jnp.roll(east_cond, 1, 1)
    south_north = jnp.roll(south_cond, 1, 0)
    diagonal = east_cond + east_west + south_cond + south_north + (leakage + PAD_GAIN * pads)
    source = (PAD_GAIN * pads[:, :, None] - load_current) / diagonal[:, :, None]
    omegas = chebyshev_weights(ITERS)
    field = source
    previous = source
    for iteration in range(ITERS):
        neighbours = east_cond[:, :, None] * jnp.roll(field, -1, 1) + east_west[:, :, None] * jnp.roll(field, 1, 1)
        neighbours = neighbours + south_cond[:, :, None] * jnp.roll(field, -1, 0)
        neighbours = neighbours + south_north[:, :, None] * jnp.roll(field, 1, 0)
        jacobi_value = source + neighbours / diagonal[:, :, None]
        if iteration == 0:
            updated = jacobi_value
        else:
            updated = omegas[iteration] * (jacobi_value - previous) + previous
        previous, field = field, updated
    return field
```

```python
import jax
import jax.numpy as jnp
from jax import lax
from jax.experimental import pallas as pl
from jax.experimental.pallas import tpu as pltpu
from jax.sharding import PartitionSpec as P

MESH = pl.DeviceIdType.MESH
PAD_GAIN = 8.0
SPECTRAL_BOUND = 0.995

N = 64
D = 4
LANE = 128
HALVES = 2
PADC = 8
ROWS = N + 2 * D
COLS = N + 2 * PADC
CHUNKS = 4
CROWS = N // CHUNKS


def polynomial():
    b2 = SPECTRAL_BOUND * SPECTRAL_BOUND
    w1 = 1.0 / (1.0 - b2 / 2.0)
    w2 = 1.0 / (1.0 - b2 * w1 / 4.0)
    w3 = 1.0 / (1.0 - b2 * w2 / 4.0)
    return w3 + (1.0 - w3) * w1, w1 * w2 * w3


ALPHA, BETA = polynomial()


def lookup(classes, table):
    value = jnp.full(classes.shape, table[0], jnp.float32)
    for label in range(1, 8):
        value = jnp.where(classes == label, table[label], value)
    return value


def lanes_of(column):
    return jnp.broadcast_to(column, (8, LANE))


def exchange_kernel(
    east_ref, south_ref, table_ref, leak_ref, pad_ref, load_hbm,
    out_ref,
    raw, rows_in, cols_in, corner_in, plain, turned, local, coef, cond, side,
    src, tee, you, vee,
    load_sem, own_sem, send_sem, recv_sem,
):
    gx, gy = lax.axis_index("gx"), lax.axis_index("gy")
    nx, ny = lax.axis_size("gx"), lax.axis_size("gy")
    up, down = lax.rem(gx + nx - 1, nx), lax.rem(gx + 1, nx)
    west, east = lax.rem(gy + ny - 1, ny), lax.rem(gy + 1, ny)

    barrier = pltpu.get_barrier_semaphore()
    around = [(up, gy), (down, gy), (gx, west), (gx, east), (up, west), (up, east), (down, west), (down, east)]
    for device in around:
        pl.semaphore_signal(barrier, inc=1, device_id=device, device_id_type=MESH)

    loads = []
    for q in range(CHUNKS):
        part = pl.ds(q * CROWS, CROWS)
        loads.append(pltpu.make_async_copy(load_hbm.at[part], raw.at[part], load_sem.at[q]))
    owns = [
        pltpu.make_async_copy(load_hbm.at[:, pl.ds(0, D), :], cols_in.at[0, :, pl.ds(D, D), :], own_sem.at[0]),
        pltpu.make_async_copy(load_hbm.at[:, pl.ds(N - D, D), :], cols_in.at[1, :, pl.ds(0, D), :], own_sem.at[1]),
    ]
    for copy in loads + owns:
        copy.start()

    table = [table_ref[label] for label in range(8)]
    pads = pad_ref[...].astype(jnp.float32)
    fields = [
        lookup(east_ref[...], table),
        lookup(south_ref[...], table),
        leak_ref[...] + PAD_GAIN * pads,
        pads,
    ]
    fill = jnp.zeros((N, LANE - N), jnp.float32)
    for a in range(4):
        plain[a, pl.ds(8, N), :] = jnp.concatenate([fields[a], fill], axis=1)

    def turn(rows):
        return jnp.transpose(rows)[0:N]

    def derive(ref, first, last):
        for e in range(first, last, 8):
            tile = pl.ds(e, 8)
            ea, so = ref[0, tile, :], ref[1, tile, :]
            we = ref[0, pl.ds(e - 1, 8), :] if e > 0 else pltpu.roll(ref[0, tile, :], 1, 0)
            no = pltpu.roll(so, 1, 1)
            inverse = 1.0 / (ea + we + so + no + ref[2, tile, :])
            for a, value in enumerate((ea, we, so, no, PAD_GAIN * ref[3, tile, :])):
                coef[a, tile, :] = value * inverse
            coef[5, tile, :] = inverse

    for a in range(4):
        middle = plain[a, pl.ds(8, N), :]
        rows = jnp.concatenate([jnp.ones((8, LANE), jnp.float32), middle, jnp.ones((56, LANE), jnp.float32)], axis=0)
        local[a, pl.ds(0, 8), :] = jnp.ones((8, LANE), jnp.float32)
        local[a, pl.ds(8, N), :] = turn(rows)
    derive(local, 8, 8 + N)

    for copy in loads + owns:
        copy.wait()
    pl.semaphore_wait(barrier, len(around))

    def remote(k, source, target, device):
        return pltpu.make_async_remote_copy(
            src_ref=source, dst_ref=target, send_sem=send_sem.at[k], recv_sem=recv_sem.at[k],
            device_id=device, device_id_type=MESH,
        )

    low, high = pl.ds(0, D), pl.ds(N - D, D)
    top3, end3 = pl.ds(0, 3), pl.ds(N - 3, 3)
    coef_x = [
        remote(0, plain.at[:, pl.ds(8, 8), :], plain.at[:, pl.ds(8 + N, 8), :], (up, gy)),
        remote(1, plain.at[:, pl.ds(N, 8), :], plain.at[:, pl.ds(0, 8), :], (down, gy)),
    ]
    bulk_x = [
        remote(2, raw.at[low], rows_in.at[1], (up, gy)),
        remote(3, raw.at[high], rows_in.at[0], (down, gy)),
    ]
    corners = [
        remote(4, raw.at[end3, high, :], corner_in.at[0], (down, east)),
        remote(5, raw.at[end3, low, :], corner_in.at[1], (down, west)),
        remote(6, raw.at[top3, high, :], corner_in.at[2], (up, east)),
        remote(7, raw.at[top3, low, :], corner_in.at[3], (up, west)),
    ]
    bulk_y = []
    for q in range(CHUNKS):
        part = pl.ds(q * CROWS, CROWS)
        bulk_y.append((
            remote(8 + q, raw.at[part, low, :], cols_in.at[1, part, pl.ds(D, D), :], (gx, west)),
            remote(12 + q, raw.at[part, high, :], cols_in.at[0, part, pl.ds(0, D), :], (gx, east)),
        ))
    coef_y = [
        remote(16, turned.at[:, pl.ds(8, 8), :], turned.at[:, pl.ds(8 + N, 8), :], (gx, west)),
        remote(17, turned.at[:, pl.ds(N, 8), :], turned.at[:, pl.ds(0, 8), :], (gx, east)),
    ]
    for copy in coef_x + [*bulk_y[0]] + bulk_x + corners + [*bulk_y[1], *bulk_y[2]]:
        copy.start()

    tiles = [8 + 8 * t for t in range(N // 8)]

    def spread_rows(base_lane, count, first_row, source_of):
        for e in tiles:
            turned_tiles = [pltpu.roll(coef[a, pl.ds(e, 8), :], base_lane, 1) for a in range(6)]
            for k in range(count):
                wide = [lanes_of(tile[:, k : k + 1]) for tile in turned_tiles]
                for a in range(4):
                    cond[a, first_row + k, pl.ds(e, 8), :] = wide[a]
                for half in range(HALVES):
                    load = source_of(k, e - 8, half)
                    if load is not None:
                        src[first_row + k, half, pl.ds(e, 8), :] = wide[4] - load * wide[5]

    def neighbours(field, weights, row, half, e):
        total = weights[0] * field[row, half, pl.ds(e + 1, 8), :]
        total = total + weights[1] * field[row, half, pl.ds(e - 1, 8), :]
        total = total + weights[2] * field[row + 1, half, pl.ds(e, 8), :]
        return total + weights[3] * field[row - 1, half, pl.ds(e, 8), :]

    def step(stage, row, columns):
        for e in columns:
            weights = [cond[a, row, pl.ds(e, 8), :] for a in range(4)]
            for half in range(HALVES):
                here = (row, half, pl.ds(e, 8), slice(None))
                if stage == 1:
                    tee[here] = src[here] + neighbours(src, weights, row, half, e)
                elif stage == 2:
                    you[here] = neighbours(tee, weights, row, half, e)
                elif stage == 3:
                    vee[here] = ALPHA * tee[here] + BETA * neighbours(you, weights, row, half, e)
                else:
                    out_ref[row - D, half, pl.ds(e, 8), :] = src[here] + neighbours(vee, weights, row, half, e)

    def sweep(stage, first, last, columns):
        def body(row, carry):
            step(stage, row, columns)
            return carry

        lax.fori_loop(first + D, last + D, body, 0)

    def own_group(g, carry):
        spread_rows(
            LANE - 8 - 8 * g, 8, D + 8 * g,
            lambda k, j, half: raw[8 * g + k, pl.ds(j, 8), pl.ds(half * LANE, LANE)],
        )
        return carry

    lax.fori_loop(0, N // 8, own_group, 0)
    sweep(1, 1, 63, tiles)
    for copy in coef_x:
        copy.wait_recv()
    for a in range(4):
        rows = jnp.concatenate([plain[a, pl.ds(0, COLS), :], jnp.ones((LANE - COLS, LANE), jnp.float32)], axis=0)
        turned[a, pl.ds(8, N), :] = turn(rows)
    sweep(2, 2, 62, tiles)
    for copy in coef_y + [*bulk_y[3]]:
        copy.start()
    sweep(3, 3, 61, tiles)
    sweep(4, 4, 60, tiles)

    for copy in coef_y:
        copy.wait_recv()
    derive(turned, 0, COLS)
    for copy in bulk_x:
        copy.wait_recv()

    def top_source(k, j, half):
        lanes = pl.ds(half * LANE, LANE)
        return rows_in[0, k, pl.ds(j, 8), lanes] if k < D else raw[k - D, pl.ds(j, 8), lanes]

    def end_source(k, j, half):
        return rows_in[1, k - D, pl.ds(j, 8), pl.ds(half * LANE, LANE)] if k >= D else None

    spread_rows(LANE - D - 0, 8, 0, top_source)
    spread_rows(LANE - D - N, 8, N, end_source)
    for stage in (1, 2, 3, 4):
        sweep(stage, stage - D, 5, tiles)
        sweep(stage, N - D, N + D - stage, tiles)

    sides = (PADC - D, PADC + N - D)

    def side_group(g, carry):
        for s, e in enumerate(sides):
            turned_tiles = [pltpu.roll(coef[a, pl.ds(e, 8), :], LANE - D - 8 * g, 1) for a in range(6)]
            for k in range(8):
                wide = [lanes_of(tile[:, k : k + 1]) for tile in turned_tiles]
                for a in range(4):
                    cond[a, 8 * g + k, pl.ds(e, 8), :] = wide[a]
                for a in range(2):
                    side[s, a, 8 * g + k] = wide[4 + a]
        return carry

    lax.fori_loop(0, ROWS // 8, side_group, 0)

    for copy in corners:
        copy.wait_recv()
    for c, (first, s, lo) in enumerate(((1, 0, 0), (1, 1, D), (D + N, 0, 0), (D + N, 1, D))):
        for k in range(3):
            for half in range(HALVES):
                load = corner_in[c, k, :, pl.ds(half * LANE, LANE)]
                gain, inverse = side[s, 0, first + k, pl.ds(lo, D), :], side[s, 1, first + k, pl.ds(lo, D), :]
                src[first + k, half, pl.ds(sides[s] + lo, D), :] = gain - load * inverse

    side_tiles = (PADC - D + 1, PADC + N - D)
    for q in range(CHUNKS):
        for copy in bulk_y[q]:
            copy.wait_recv()

        def side_source(row, carry):
            for s, e in enumerate(sides):
                for half in range(HALVES):
                    load = cols_in[s, row, :, pl.ds(half * LANE, LANE)]
                    src[row + D, half, pl.ds(e, 8), :] = side[s, 0, row + D] - load * side[s, 1, row + D]
            return carry

        lax.fori_loop(q * CROWS, (q + 1) * CROWS, side_source, 0)
        for stage in (1, 2, 3, 4):
            first = stage - D if q == 0 else q * CROWS - stage
            last = N + D - stage if q == CHUNKS - 1 else (q + 1) * CROWS - stage
            sweep(stage, first, last, side_tiles)

    for copy in coef_x + bulk_x + corners + coef_y + [c for pair in bulk_y for c in pair]:
        copy.wait_send()


def store_kernel(field, out_hbm, sem):
    copies = []
    for q in range(CHUNKS):
        for half in range(HALVES):
            part = pl.ds(q * CROWS, CROWS)
            copies.append(pltpu.make_async_copy(
                field.at[part, half, pl.ds(PADC, N), :],
                out_hbm.at[part, :, pl.ds(half * LANE, LANE)],
                sem.at[q, half],
            ))
    for copy in copies:
        copy.start()
    for copy in copies:
        copy.wait()


def body(east_class, south_class, cond_table, leakage, pad_mask, load_current):
    vmem = pl.BlockSpec(memory_space=pltpu.VMEM)
    f32 = jnp.float32
    width = HALVES * LANE
    field = pltpu.VMEM((ROWS, HALVES, COLS, LANE), f32)
    inside = pl.pallas_call(
        exchange_kernel,
        out_shape=jax.ShapeDtypeStruct((N, HALVES, COLS, LANE), f32),
        in_specs=[vmem, vmem, pl.BlockSpec(memory_space=pltpu.SMEM), vmem, vmem, pl.BlockSpec(memory_space=pltpu.HBM)],
        out_specs=vmem,
        scratch_shapes=[
            pltpu.VMEM((N, N, width), f32),
            pltpu.VMEM((2, D, N, width), f32),
            pltpu.VMEM((2, N, 2 * D, width), f32),
            pltpu.VMEM((4, 3, D, width), f32),
            pltpu.VMEM((4, COLS, LANE), f32),
            pltpu.VMEM((4, COLS, LANE), f32),
            pltpu.VMEM((4, COLS, LANE), f32),
            pltpu.VMEM((6, COLS, LANE), f32),
            pltpu.VMEM((4, ROWS, COLS, LANE), f32),
            pltpu.VMEM((2, 2, ROWS, 8, LANE), f32),
            field, field, field, field,
            pltpu.SemaphoreType.DMA((CHUNKS,)),
            pltpu.SemaphoreType.DMA((2,)),
            pltpu.SemaphoreType.DMA((18,)),
            pltpu.SemaphoreType.DMA((18,)),
        ],
        compiler_params=pltpu.CompilerParams(collective_id=0, has_side_effects=True, vmem_limit_bytes=44 << 20),
        name="exchange",
    )(east_class, south_class, cond_table, leakage, pad_mask, pltpu.with_memory_space_constraint(load_current, pltpu.HBM))
    return pl.pallas_call(
        store_kernel,
        out_shape=jax.ShapeDtypeStruct((N, N, width), f32),
        in_specs=[vmem],
        out_specs=pl.BlockSpec(memory_space=pltpu.HBM),
        scratch_shapes=[pltpu.SemaphoreType.DMA((CHUNKS, HALVES))],
        compiler_params=pltpu.CompilerParams(vmem_limit_bytes=8 << 20),
        name="store",
    )(inside)


def solution(mesh):
    block = P("gx", "gy")
    return jax.shard_map(
        body,
        mesh=mesh,
        in_specs=(block, block, P(), block, block, P("gx", "gy", None)),
        out_specs=P("gx", "gy", None),
        check_vma=False,
    )
```

```python
import jax
import jax.numpy as jnp
from jax import lax
from jax.experimental import pallas as pl
from jax.experimental.pallas import tpu as pltpu
from jax.sharding import PartitionSpec as P

MESH = pl.DeviceIdType.MESH
PAD_GAIN = 8.0
SPECTRAL_BOUND = 0.995

N = 64
D = 4
LANE = 128
HALVES = 2
PADC = 8
ROWS = N + 2 * D
COLS = N + 2 * PADC
CHUNKS = 4
CROWS = N // CHUNKS


def polynomial():
    b2 = SPECTRAL_BOUND * SPECTRAL_BOUND
    w1 = 1.0 / (1.0 - b2 / 2.0)
    w2 = 1.0 / (1.0 - b2 * w1 / 4.0)
    w3 = 1.0 / (1.0 - b2 * w2 / 4.0)
    return w3 + (1.0 - w3) * w1, w1 * w2 * w3


ALPHA, BETA = polynomial()


def lookup(classes, table):
    value = jnp.full(classes.shape, table[0], jnp.float32)
    for label in range(1, 8):
        value = jnp.where(classes == label, table[label], value)
    return value


def pick_lane(tile, lane):
    return jnp.take_along_axis(tile, lane, axis=1, mode="promise_in_bounds")


def exchange_kernel(
    east_hbm, south_hbm, table_hbm, leak_hbm, pad_hbm, load_hbm,
    out_ref,
    east_ref, south_ref, leak_ref, pad_ref, table_ref,
    raw, rows_in, cols_in, corner_in, plain, turned, local, coef, cond,
    src, tee, you, vee,
    load_sem, own_sem, input_sem, send_sem, recv_sem, ready_sem,
):
    gx, gy = lax.axis_index("gx"), lax.axis_index("gy")
    nx, ny = lax.axis_size("gx"), lax.axis_size("gy")
    up, down = lax.rem(gx + nx - 1, nx), lax.rem(gx + 1, nx)
    west, east = lax.rem(gy + ny - 1, ny), lax.rem(gy + 1, ny)

    odd = lax.rem(gy, 2)
    near, cross = odd * west + (1 - odd) * east, odd * east + (1 - odd) * west
    early = gy // 2 < cross // 2
    late = jnp.logical_not(early)
    is_odd, is_even = odd == 1, odd == 0

    barrier = pltpu.get_barrier_semaphore()

    def signal(semaphore, devices):
        for device in devices:
            pl.semaphore_signal(semaphore, inc=1, device_id=device, device_id_type=MESH)

    across = [(gx, cross), (up, cross), (down, cross)]
    signal(barrier, [(up, gy), (down, gy), (gx, near), (up, near), (down, near)])

    @pl.when(early)
    def _():
        signal(barrier, across)

    inputs = [
        pltpu.make_async_copy(hbm, ref, input_sem.at[k])
        for k, (hbm, ref) in enumerate((
            (east_hbm, east_ref), (south_hbm, south_ref), (leak_hbm, leak_ref), (pad_hbm, pad_ref), (table_hbm, table_ref),
        ))
    ]
    loads = []
    for q in range(CHUNKS):
        part = pl.ds(q * CROWS, CROWS)
        loads.append(pltpu.make_async_copy(load_hbm.at[part], raw.at[part], load_sem.at[q]))
    owns = [
        pltpu.make_async_copy(load_hbm.at[:, pl.ds(0, D), :], cols_in.at[0, :, pl.ds(D, D), :], own_sem.at[0]),
        pltpu.make_async_copy(load_hbm.at[:, pl.ds(N - D, D), :], cols_in.at[1, :, pl.ds(0, D), :], own_sem.at[1]),
    ]
    for copy in inputs + loads + owns:
        copy.start()
    for copy in inputs:
        copy.wait()

    table = [table_ref[label] for label in range(8)]
    pads = pad_ref[...].astype(jnp.float32)
    fields = [
        lookup(east_ref[...], table),
        lookup(south_ref[...], table),
        leak_ref[...] + PAD_GAIN * pads,
        pads,
    ]
    fill = jnp.zeros((N, LANE - N), jnp.float32)
    for a in range(4):
        plain[a, pl.ds(8, N), :] = jnp.concatenate([fields[a], fill], axis=1)

    for copy in loads:
        copy.wait()
    pl.semaphore_wait(barrier, 5 + 3 * late.astype(jnp.int32))

    def remote(k, source, target, device):
        return pltpu.make_async_remote_copy(
            src_ref=source, dst_ref=target, send_sem=send_sem.at[k], recv_sem=recv_sem.at[k],
            device_id=device, device_id_type=MESH,
        )

    low, high = pl.ds(0, D), pl.ds(N - D, D)
    top3, end3 = pl.ds(0, 3), pl.ds(N - 3, 3)
    coef_x = [
        remote(0, plain.at[:, pl.ds(8, 8), :], plain.at[:, pl.ds(8 + N, 8), :], (up, gy)),
        remote(1, plain.at[:, pl.ds(N, 8), :], plain.at[:, pl.ds(0, 8), :], (down, gy)),
    ]
    bulk_x = [
        remote(2, raw.at[low], rows_in.at[1], (up, gy)),
        remote(3, raw.at[high], rows_in.at[0], (down, gy)),
    ]
    corners = [
        [
            remote(4, raw.at[end3, high, :], corner_in.at[0], (down, east)),
            remote(6, raw.at[top3, high, :], corner_in.at[2], (up, east)),
        ],
        [
            remote(5, raw.at[end3, low, :], corner_in.at[1], (down, west)),
            remote(7, raw.at[top3, low, :], corner_in.at[3], (up, west)),
        ],
    ]
    bulk_y = [[], []]
    for q in range(CHUNKS):
        part = pl.ds(q * CROWS, CROWS)
        bulk_y[0].append(remote(8 + q, raw.at[part, high, :], cols_in.at[0, part, pl.ds(0, D), :], (gx, east)))
        bulk_y[1].append(remote(12 + q, raw.at[part, low, :], cols_in.at[1, part, pl.ds(D, D), :], (gx, west)))
    coef_y = [
        remote(16, turned.at[:, pl.ds(N, 8), :], turned.at[:, pl.ds(0, 8), :], (gx, east)),
        remote(17, turned.at[:, pl.ds(8, 8), :], turned.at[:, pl.ds(8 + N, 8), :], (gx, west)),
    ]

    def send(way, first, last):
        for copy in bulk_y[way][first:last] + (corners[way] if first == 0 else []):
            copy.start()

    @pl.when(late)
    def _():
        signal(ready_sem, across)

    for copy in coef_x + bulk_x:
        copy.start()

    @pl.when(jnp.logical_and(early, is_odd))
    def _():
        send(1, 0, CHUNKS)

    @pl.when(jnp.logical_and(early, is_even))
    def _():
        send(0, 0, CHUNKS)

    @pl.when(jnp.logical_and(late, is_odd))
    def _():
        send(0, 0, CHUNKS)
        send(1, 0, 2)

    @pl.when(jnp.logical_and(late, is_even))
    def _():
        send(1, 0, CHUNKS)
        send(0, 0, 2)

    def turn(rows):
        return jnp.transpose(rows)[0:N]

    def derive(ref, first, last):
        for e in range(first, last, 8):
            tile = pl.ds(e, 8)
            ea, so = ref[0, tile, :], ref[1, tile, :]
            we = ref[0, pl.ds(e - 1, 8), :] if e > 0 else pltpu.roll(ref[0, tile, :], 1, 0)
            no = pltpu.roll(so, 1, 1)
            inverse = 1.0 / (ea + we + so + no + ref[2, tile, :])
            for a, value in enumerate((ea, so, PAD_GAIN * ref[3, tile, :] * inverse, inverse)):
                coef[a, tile, :] = value

    for a in range(4):
        middle = plain[a, pl.ds(8, N), :]
        rows = jnp.concatenate([jnp.ones((8, LANE), jnp.float32), middle, jnp.ones((56, LANE), jnp.float32)], axis=0)
        local[a, pl.ds(0, 8), :] = jnp.ones((8, LANE), jnp.float32)
        local[a, pl.ds(8, N), :] = turn(rows)
    derive(local, 8, 8 + N)

    tiles = [8 + 8 * t for t in range(N // 8)]

    def spread(row, columns, source_of):
        lane = jnp.full((8, LANE), row + D, jnp.int32)
        for e in columns:
            wide = [pick_lane(coef[a, pl.ds(e, 8), :], lane) for a in range(4)]
            for a in range(4):
                cond[row, a, pl.ds(e, 8), :] = wide[a]
            if source_of is not None:
                for half in range(HALVES):
                    src[row, half, pl.ds(e, 8), :] = wide[2] - source_of(row, e - 8, half) * wide[3]

    def step(stage, row, columns):
        for e in columns:
            here, before = pl.ds(e, 8), pl.ds(e - 1, 8)
            ea, we = cond[row, 0, here, :], cond[row, 0, before, :]
            so, no = cond[row, 1, here, :], cond[row - 1, 1, here, :]
            inverse = cond[row, 3, here, :]
            if stage == 3:
                inverse = inverse * BETA
            field = (src, tee, you, vee)[stage - 1]
            for half in range(HALVES):
                total = ea * field[row, half, pl.ds(e + 1, 8), :] + we * field[row, half, before, :]
                total = total + (so * field[row + 1, half, here, :] + no * field[row - 1, half, here, :])
                total = total * inverse
                if stage == 1:
                    tee[row, half, here, :] = src[row, half, here, :] + total
                elif stage == 2:
                    you[row, half, here, :] = total
                elif stage == 3:
                    vee[row, half, here, :] = ALPHA * tee[row, half, here, :] + total
                else:
                    out_ref[row - D, half, here, :] = src[row, half, here, :] + total

    def rows_loop(first, last, unroll, work):
        blocks = (last - first) // unroll

        def body(block, carry):
            for k in range(unroll):
                work(first + D + block * unroll + k)
            return carry

        lax.fori_loop(0, blocks, body, 0)
        for row in range(first + blocks * unroll, last):
            work(row + D)

    def sweep(stage, first, last, columns, unroll=1):
        rows_loop(first, last, unroll, lambda row: step(stage, row, columns))

    rows_loop(0, N, 2, lambda row: spread(
        row, tiles, lambda r, j, half: raw[r - D, pl.ds(j, 8), pl.ds(half * LANE, LANE)]))
    sweep(1, 1, 63, tiles)
    for copy in coef_x:
        copy.wait_recv()
    for a in range(4):
        rows = jnp.concatenate([plain[a, pl.ds(0, COLS), :], jnp.ones((LANE - COLS, LANE), jnp.float32)], axis=0)
        turned[a, pl.ds(8, N), :] = turn(rows)
    sweep(2, 2, 62, tiles)

    @pl.when(early)
    def _():
        pl.semaphore_wait(ready_sem, len(across))

    for copy in coef_y:
        copy.start()

    @pl.when(jnp.logical_and(early, is_odd))
    def _():
        send(0, 0, CHUNKS)

    @pl.when(jnp.logical_and(early, is_even))
    def _():
        send(1, 0, CHUNKS)

    @pl.when(jnp.logical_and(late, is_odd))
    def _():
        send(1, 2, CHUNKS)

    @pl.when(jnp.logical_and(late, is_even))
    def _():
        send(0, 2, CHUNKS)

    sweep(3, 3, 61, tiles)
    sweep(4, 4, 60, tiles)

    for copy in coef_y + bulk_x:
        copy.wait_recv()
    derive(turned, 0, COLS)
    rows_loop(-D, 0, 1, lambda row: spread(
        row, tiles, lambda r, j, half: rows_in[0, r, pl.ds(j, 8), pl.ds(half * LANE, LANE)]))
    rows_loop(0, 1, 1, lambda row: spread(
        row, tiles, lambda r, j, half: raw[r - D, pl.ds(j, 8), pl.ds(half * LANE, LANE)]))
    rows_loop(N, N + D, 1, lambda row: spread(
        row, tiles, lambda r, j, half: rows_in[1, r - N - D, pl.ds(j, 8), pl.ds(half * LANE, LANE)]))
    for stage in (1, 2, 3, 4):
        sweep(stage, stage - D, 5, tiles)
        sweep(stage, N - D, N + D - stage, tiles)

    rows_loop(-D, N + D, 4, lambda row: spread(row, (PADC - D, PADC + N - D), None))
    for copy in owns:
        copy.wait()

    def arrived(side, copies):
        for way in range(2):
            @pl.when(side == way)
            def _(way=way):
                for copy in copies[way]:
                    copy.wait_recv()

    def do_side(side):
        halo = PADC - D + side * N
        tile = PADC - D + 1 + side * (N - 1)
        ghost = PADC - D + side * (N + D)
        for q in range(CHUNKS):
            arrived(side, [[bulk_y[way][q]] + (corners[way] if q == 0 else []) for way in range(2)])
            if q == 0:
                for c, first in ((0, 1), (2, D + N)):
                    for k in range(3):
                        for half in range(HALVES):
                            load = corner_in[c + side, k, :, pl.ds(half * LANE, LANE)]
                            gain, inverse = cond[first + k, 2, pl.ds(ghost, D), :], cond[first + k, 3, pl.ds(ghost, D), :]
                            src[first + k, half, pl.ds(ghost, D), :] = gain - load * inverse

            def side_source(row):
                gain, inverse = cond[row, 2, pl.ds(halo, 8), :], cond[row, 3, pl.ds(halo, 8), :]
                for half in range(HALVES):
                    load = cols_in[side, row - D, :, pl.ds(half * LANE, LANE)]
                    src[row, half, pl.ds(halo, 8), :] = gain - load * inverse

            rows_loop(q * CROWS, (q + 1) * CROWS, 4, side_source)
            for stage in (1, 2, 3, 4):
                first = stage - D if q == 0 else q * CROWS - stage
                last = N + D - stage if q == CHUNKS - 1 else (q + 1) * CROWS - stage
                sweep(stage, first, last, (tile,), 4)

    do_side(1 - odd)
    do_side(odd)

    for copy in coef_x + bulk_x + coef_y + corners[0] + corners[1] + bulk_y[0] + bulk_y[1]:
        copy.wait_send()


def store_kernel(field, out_hbm, sem):
    copies = []
    for q in range(CHUNKS):
        for half in range(HALVES):
            part = pl.ds(q * CROWS, CROWS)
            copies.append(pltpu.make_async_copy(
                field.at[part, half, pl.ds(PADC, N), :],
                out_hbm.at[part, :, pl.ds(half * LANE, LANE)],
                sem.at[q, half],
            ))
    for copy in copies:
        copy.start()
    for copy in copies:
        copy.wait()


def body(east_class, south_class, cond_table, leakage, pad_mask, load_current):
    vmem, hbm = pl.BlockSpec(memory_space=pltpu.VMEM), pl.BlockSpec(memory_space=pltpu.HBM)
    f32 = jnp.float32
    width = HALVES * LANE
    field = pltpu.VMEM((ROWS, HALVES, COLS, LANE), f32)
    inside = pl.pallas_call(
        exchange_kernel,
        out_shape=jax.ShapeDtypeStruct((N, HALVES, COLS, LANE), f32),
        in_specs=[hbm] * 6,
        out_specs=vmem,
        scratch_shapes=[
            pltpu.VMEM((N, N), jnp.int32),
            pltpu.VMEM((N, N), jnp.int32),
            pltpu.VMEM((N, N), f32),
            pltpu.VMEM((N, N), jnp.int32),
            pltpu.SMEM((8,), f32),
            pltpu.VMEM((N, N, width), f32),
            pltpu.VMEM((2, D, N, width), f32),
            pltpu.VMEM((2, N, 2 * D, width), f32),
            pltpu.VMEM((4, 3, D, width), f32),
            pltpu.VMEM((4, COLS, LANE), f32),
            pltpu.VMEM((4, COLS, LANE), f32),
            pltpu.VMEM((4, COLS, LANE), f32),
            pltpu.VMEM((4, COLS, LANE), f32),
            pltpu.VMEM((ROWS, 4, COLS, LANE), f32),
            field, field, field, field,
            pltpu.SemaphoreType.DMA((CHUNKS,)),
            pltpu.SemaphoreType.DMA((2,)),
            pltpu.SemaphoreType.DMA((5,)),
            pltpu.SemaphoreType.DMA((18,)),
            pltpu.SemaphoreType.DMA((18,)),
            pltpu.SemaphoreType.REGULAR,
        ],
        compiler_params=pltpu.CompilerParams(collective_id=0, has_side_effects=True, vmem_limit_bytes=44 << 20),
        name="exchange",
    )(*(pltpu.with_memory_space_constraint(array, pltpu.HBM) for array in (
        east_class, south_class, cond_table, leakage, pad_mask, load_current)))
    return pl.pallas_call(
        store_kernel,
        out_shape=jax.ShapeDtypeStruct((N, N, width), f32),
        in_specs=[vmem],
        out_specs=pl.BlockSpec(memory_space=pltpu.HBM),
        scratch_shapes=[pltpu.SemaphoreType.DMA((CHUNKS, HALVES))],
        compiler_params=pltpu.CompilerParams(vmem_limit_bytes=8 << 20),
        name="store",
    )(inside)


def solution(mesh):
    block = P("gx", "gy")
    return jax.shard_map(
        body,
        mesh=mesh,
        in_specs=(block, block, P(), block, block, P("gx", "gy", None)),
        out_specs=P("gx", "gy", None),
        check_vma=False,
    )
```

```python
import jax
import jax.numpy as jnp
from jax import lax
from jax.experimental import pallas as pl
from jax.experimental.pallas import tpu as pltpu
from jax.sharding import PartitionSpec as P

MESH = pl.DeviceIdType.MESH
PAD_GAIN = 8.0
SPECTRAL_BOUND = 0.995

N = 64
D = 4
LANE = 128
HALVES = 2
PADC = 8
ROWS = N + 2 * D
COLS = N + 2 * PADC
CHUNKS = 4
CROWS = N // CHUNKS


def polynomial():
    b2 = SPECTRAL_BOUND * SPECTRAL_BOUND
    w1 = 1.0 / (1.0 - b2 / 2.0)
    w2 = 1.0 / (1.0 - b2 * w1 / 4.0)
    w3 = 1.0 / (1.0 - b2 * w2 / 4.0)
    return w3 + (1.0 - w3) * w1, w1 * w2 * w3


ALPHA, BETA = polynomial()


def lookup(classes, table):
    value = jnp.full(classes.shape, table[0], jnp.float32)
    for label in range(1, 8):
        value = jnp.where(classes == label, table[label], value)
    return value


def pick_lane(tile, lane):
    return jnp.take_along_axis(tile, lane, axis=1, mode="promise_in_bounds")


def exchange_kernel(
    east_hbm, south_hbm, table_hbm, leak_hbm, pad_hbm, load_hbm,
    out_ref,
    east_ref, south_ref, leak_ref, pad_ref, table_ref,
    raw, rows_in, cols_in, corner_in, plain, turned, coef, coef_side, cond,
    src, tee, you, vee,
    load_sem, own_sem, input_sem, send_sem, recv_sem, ready_sem,
):
    gx, gy = lax.axis_index("gx"), lax.axis_index("gy")
    nx, ny = lax.axis_size("gx"), lax.axis_size("gy")
    up, down = lax.rem(gx + nx - 1, nx), lax.rem(gx + 1, nx)
    west, east = lax.rem(gy + ny - 1, ny), lax.rem(gy + 1, ny)

    odd = lax.rem(gy, 2)
    near, cross = odd * west + (1 - odd) * east, odd * east + (1 - odd) * west
    early = gy // 2 < cross // 2
    late = jnp.logical_not(early)
    is_odd, is_even = odd == 1, odd == 0

    barrier = pltpu.get_barrier_semaphore()

    def signal(semaphore, devices):
        for device in devices:
            pl.semaphore_signal(semaphore, inc=1, device_id=device, device_id_type=MESH)

    across = [(gx, cross), (up, cross), (down, cross)]
    signal(barrier, [(up, gy), (down, gy), (gx, near), (up, near), (down, near)])

    @pl.when(early)
    def _():
        signal(barrier, across)

    inputs = [
        pltpu.make_async_copy(hbm, ref, input_sem.at[k])
        for k, (hbm, ref) in enumerate((
            (east_hbm, east_ref), (south_hbm, south_ref), (leak_hbm, leak_ref), (pad_hbm, pad_ref), (table_hbm, table_ref),
        ))
    ]
    loads = []
    for q in range(CHUNKS):
        part = pl.ds(q * CROWS, CROWS)
        loads.append(pltpu.make_async_copy(load_hbm.at[part], raw.at[part], load_sem.at[q]))
    owns = [
        pltpu.make_async_copy(load_hbm.at[:, pl.ds(0, D), :], cols_in.at[0, :, pl.ds(D, D), :], own_sem.at[0]),
        pltpu.make_async_copy(load_hbm.at[:, pl.ds(N - D, D), :], cols_in.at[1, :, pl.ds(0, D), :], own_sem.at[1]),
    ]
    for copy in inputs + loads + owns:
        copy.start()
    for copy in inputs:
        copy.wait()

    table = [table_ref[label] for label in range(8)]
    pads = pad_ref[...].astype(jnp.float32)
    fields = [
        lookup(east_ref[...], table),
        lookup(south_ref[...], table),
        leak_ref[...] + PAD_GAIN * pads,
        pads,
    ]
    fill = jnp.zeros((N, LANE - N), jnp.float32)
    for a in range(4):
        plain[a, pl.ds(8, N), :] = jnp.concatenate([fields[a], fill], axis=1)

    def turn(rows):
        return jnp.transpose(rows)[0:N]

    column = lax.broadcasted_iota(jnp.int32, (N, LANE), 0)

    def derive(blocks):
        ea, so, extra, pad = (turn(rows) for rows in blocks)
        diagonal = ea + jnp.where(column == 0, 0.0, pltpu.roll(ea, 1, 0)) + so + pltpu.roll(so, 1, 1) + extra
        inverse = 1.0 / diagonal
        for a, value in enumerate((ea, so, PAD_GAIN * pad * inverse, inverse)):
            coef[a] = value
        return ea, so, diagonal, pad

    ones = jnp.ones((8, LANE), jnp.float32)
    tail = jnp.ones((LANE - 8 - N, LANE), jnp.float32)
    derive([jnp.concatenate([ones, jnp.concatenate([field, fill], axis=1), tail], axis=0) for field in fields])

    for copy in loads:
        copy.wait()
    pl.semaphore_wait(barrier, 5 + 3 * late.astype(jnp.int32))

    def remote(k, source, target, device):
        return pltpu.make_async_remote_copy(
            src_ref=source, dst_ref=target, send_sem=send_sem.at[k], recv_sem=recv_sem.at[k],
            device_id=device, device_id_type=MESH,
        )

    low, high = pl.ds(0, D), pl.ds(N - D, D)
    coef_x = [
        remote(0, plain.at[:, pl.ds(8, 8), :], plain.at[:, pl.ds(8 + N, 8), :], (up, gy)),
        remote(1, plain.at[:, pl.ds(N, 8), :], plain.at[:, pl.ds(0, 8), :], (down, gy)),
    ]
    bulk_x = [
        remote(2, raw.at[low], rows_in.at[1], (up, gy)),
        remote(3, raw.at[high], rows_in.at[0], (down, gy)),
    ]
    corners = [[], []]
    for k in range(3):
        size = 4 if k == 2 else 2
        wide = pl.ds(N - size, size), pl.ds(0, size)
        for c, (row, device) in enumerate(((N - 3 + k, down), (2 - k, up))):
            land = k if c == 0 else 2 - k
            corners[0].append(remote(18 + 6 * c + k, raw.at[row, wide[0], :], corner_in.at[2 * c, land, pl.ds(D - size, size), :], (device, east)))
            corners[1].append(remote(21 + 6 * c + k, raw.at[row, wide[1], :], corner_in.at[2 * c + 1, land, pl.ds(0, size), :], (device, west)))
    bulk_y = [[], []]
    for q in range(CHUNKS):
        part = pl.ds(q * CROWS, CROWS)
        bulk_y[0].append(remote(8 + q, raw.at[part, high, :], cols_in.at[0, part, pl.ds(0, D), :], (gx, east)))
        bulk_y[1].append(remote(12 + q, raw.at[part, low, :], cols_in.at[1, part, pl.ds(D, D), :], (gx, west)))
    coef_y = [
        remote(16, turned.at[:, pl.ds(PADC + N - D, D), :], turned.at[:, pl.ds(PADC - D, D), :], (gx, east)),
        remote(17, turned.at[:, pl.ds(PADC, D), :], turned.at[:, pl.ds(PADC + N, D), :], (gx, west)),
    ]

    def send(way, first, last):
        for copy in bulk_y[way][first:last] + (corners[way] if first == 0 else []):
            copy.start()

    @pl.when(late)
    def _():
        signal(ready_sem, across)

    for copy in coef_x + bulk_x:
        copy.start()

    @pl.when(jnp.logical_and(early, is_odd))
    def _():
        send(1, 0, CHUNKS)

    @pl.when(jnp.logical_and(early, is_even))
    def _():
        send(0, 0, CHUNKS)

    @pl.when(jnp.logical_and(late, is_odd))
    def _():
        send(0, 0, CHUNKS)
        send(1, 0, 2)

    @pl.when(jnp.logical_and(late, is_even))
    def _():
        send(1, 0, CHUNKS)
        send(0, 0, 2)

    tiles = [8 + 8 * t for t in range(N // 8)]

    def spread(row, source_of):
        lane = jnp.full((8, LANE), row + D, jnp.int32)
        for e in tiles:
            wide = [pick_lane(coef[a, pl.ds(e - PADC, 8), :], lane) for a in range(4)]
            for a in range(4):
                cond[row, a, pl.ds(e, 8), :] = wide[a]
            for half in range(HALVES):
                src[row, half, pl.ds(e, 8), :] = wide[2] - source_of(row, e - 8, half) * wide[3]

    def spread_side(row):
        lane = jnp.full((8, LANE), row + D, jnp.int32)
        for side, e in enumerate((PADC - D, PADC + N - D)):
            for a in range(4):
                cond[row, a, pl.ds(e, 8), :] = pick_lane(coef_side[side, a], lane)

    def step(stage, row, columns):
        for e in columns:
            here, before = pl.ds(e, 8), pl.ds(e - 1, 8)
            ea, we = cond[row, 0, here, :], cond[row, 0, before, :]
            so, no = cond[row, 1, here, :], cond[row - 1, 1, here, :]
            inverse = cond[row, 3, here, :]
            if stage == 3:
                inverse = inverse * BETA
            field = (src, tee, you, vee)[stage - 1]
            for half in range(HALVES):
                total = ea * field[row, half, pl.ds(e + 1, 8), :] + we * field[row, half, before, :]
                total = total + (so * field[row + 1, half, here, :] + no * field[row - 1, half, here, :])
                total = total * inverse
                if stage == 1:
                    tee[row, half, here, :] = src[row, half, here, :] + total
                elif stage == 2:
                    you[row, half, here, :] = total
                elif stage == 3:
                    vee[row, half, here, :] = ALPHA * tee[row, half, here, :] + total
                else:
                    out_ref[row - D, half, here, :] = src[row, half, here, :] + total

    def rows_loop(first, last, unroll, work):
        blocks = (last - first) // unroll

        def body(block, carry):
            for k in range(unroll):
                work(first + D + block * unroll + k)
            return carry

        lax.fori_loop(0, blocks, body, 0)
        for row in range(first + blocks * unroll, last):
            work(row + D)

    def sweep(stage, first, last, columns, unroll=1):
        rows_loop(first, last, unroll, lambda row: step(stage, row, columns))

    def own_load(r, j, half):
        return raw[r - D, pl.ds(j, 8), pl.ds(half * LANE, LANE)]

    rows_loop(0, N // 2, 2, lambda row: spread(row, own_load))
    for copy in coef_x:
        copy.wait_recv()
    for a, value in enumerate(derive(
            [jnp.concatenate([plain[a, pl.ds(0, COLS), :], tail[0 : LANE - COLS]], axis=0) for a in range(4)])):
        turned[a, pl.ds(PADC, N), :] = value
    rows_loop(N // 2, N, 2, lambda row: spread(row, own_load))

    @pl.when(early)
    def _():
        pl.semaphore_wait(ready_sem, len(across))

    for copy in coef_y:
        copy.start()

    @pl.when(jnp.logical_and(early, is_odd))
    def _():
        send(0, 0, CHUNKS)

    @pl.when(jnp.logical_and(early, is_even))
    def _():
        send(1, 0, CHUNKS)

    @pl.when(jnp.logical_and(late, is_odd))
    def _():
        send(1, 2, CHUNKS)

    @pl.when(jnp.logical_and(late, is_even))
    def _():
        send(0, 2, CHUNKS)

    sweep(1, 1, 63, tiles)
    sweep(2, 2, 62, tiles)
    sweep(3, 3, 61, tiles)
    sweep(4, 4, 60, tiles)

    for copy in bulk_x:
        copy.wait_recv()
    rows_loop(-D, 0, 2, lambda row: spread(
        row, lambda r, j, half: rows_in[0, r, pl.ds(j, 8), pl.ds(half * LANE, LANE)]))
    rows_loop(0, 1, 1, lambda row: spread(row, own_load))
    rows_loop(N, N + D, 2, lambda row: spread(
        row, lambda r, j, half: rows_in[1, r - N - D, pl.ds(j, 8), pl.ds(half * LANE, LANE)]))
    for stage in (1, 2, 3, 4):
        sweep(stage, stage - D, 5, tiles)
        sweep(stage, N - D, N + D - stage, tiles)

    for copy in coef_y:
        copy.wait_recv()
    place = lax.broadcasted_iota(jnp.int32, (8, LANE), 0)
    for side in range(2):
        ea, so, diagonal, pad = (turned[a, pl.ds(PADC - D + side * N, 8), :] for a in range(4))
        inverse = 1.0 / (diagonal + jnp.where(place == D, pltpu.roll(ea, 1, 0), 0.0))
        for a, value in enumerate((ea, so, PAD_GAIN * pad * inverse, inverse)):
            coef_side[side, a] = value
    rows_loop(-D, N + D, 4, spread_side)
    for copy in owns:
        copy.wait()
    first = pl.ds(PADC, D)
    for c, top in enumerate((0, D + N)):
        for k in range(D):
            gain, inverse = cond[top + k, 2, first, :], cond[top + k, 3, first, :]
            for half in range(HALVES):
                load = rows_in[c, k, pl.ds(0, D), pl.ds(half * LANE, LANE)]
                src[top + k, half, first, :] = gain - load * inverse

    def arrived(side, copies):
        for way in range(2):
            @pl.when(side == way)
            def _(way=way):
                for copy in copies[way]:
                    copy.wait_recv()

    def do_side(side):
        halo = PADC - D + side * N
        tile = PADC - D + 1 + side * (N - 1)
        ghost = PADC - D + side * (N + D)
        for q in range(CHUNKS):
            arrived(side, [[bulk_y[way][q]] + (corners[way] if q == 0 else []) for way in range(2)])
            if q == 0:
                for c, first in ((0, 1), (2, D + N)):
                    for k in range(3):
                        for half in range(HALVES):
                            load = corner_in[c + side, k, :, pl.ds(half * LANE, LANE)]
                            gain, inverse = cond[first + k, 2, pl.ds(ghost, D), :], cond[first + k, 3, pl.ds(ghost, D), :]
                            src[first + k, half, pl.ds(ghost, D), :] = gain - load * inverse

            def side_source(row):
                gain, inverse = cond[row, 2, pl.ds(halo, 8), :], cond[row, 3, pl.ds(halo, 8), :]
                for half in range(HALVES):
                    load = cols_in[side, row - D, :, pl.ds(half * LANE, LANE)]
                    src[row, half, pl.ds(halo, 8), :] = gain - load * inverse

            rows_loop(q * CROWS, (q + 1) * CROWS, 8, side_source)
            for stage in (1, 2, 3, 4):
                first = stage - D if q == 0 else q * CROWS - stage
                last = N + D - stage if q == CHUNKS - 1 else (q + 1) * CROWS - stage
                sweep(stage, first, last, (tile,), 8)

    do_side(1 - odd)
    do_side(odd)

    for copy in coef_x + bulk_x + coef_y + corners[0] + corners[1] + bulk_y[0] + bulk_y[1]:
        copy.wait_send()


def store_kernel(field, out_hbm, sem):
    copies = []
    for q in range(CHUNKS):
        for half in range(HALVES):
            part = pl.ds(q * CROWS, CROWS)
            copies.append(pltpu.make_async_copy(
                field.at[part, half, pl.ds(PADC, N), :],
                out_hbm.at[part, :, pl.ds(half * LANE, LANE)],
                sem.at[q, half],
            ))
    for copy in copies:
        copy.start()
    for copy in copies:
        copy.wait()


def body(east_class, south_class, cond_table, leakage, pad_mask, load_current):
    vmem, hbm = pl.BlockSpec(memory_space=pltpu.VMEM), pl.BlockSpec(memory_space=pltpu.HBM)
    f32 = jnp.float32
    width = HALVES * LANE
    field = pltpu.VMEM((ROWS, HALVES, COLS, LANE), f32)
    inside = pl.pallas_call(
        exchange_kernel,
        out_shape=jax.ShapeDtypeStruct((N, HALVES, COLS, LANE), f32),
        in_specs=[hbm] * 6,
        out_specs=vmem,
        scratch_shapes=[
            pltpu.VMEM((N, N), jnp.int32),
            pltpu.VMEM((N, N), jnp.int32),
            pltpu.VMEM((N, N), f32),
            pltpu.VMEM((N, N), jnp.int32),
            pltpu.SMEM((8,), f32),
            pltpu.VMEM((N, N, width), f32),
            pltpu.VMEM((2, D, N, width), f32),
            pltpu.VMEM((2, N, 2 * D, width), f32),
            pltpu.VMEM((4, 3, D, width), f32),
            pltpu.VMEM((4, COLS, LANE), f32),
            pltpu.VMEM((4, COLS, LANE), f32),
            pltpu.VMEM((4, N, LANE), f32),
            pltpu.VMEM((2, 4, 8, LANE), f32),
            pltpu.VMEM((ROWS, 4, COLS, LANE), f32),
            field, field, field, field,
            pltpu.SemaphoreType.DMA((CHUNKS,)),
            pltpu.SemaphoreType.DMA((2,)),
            pltpu.SemaphoreType.DMA((5,)),
            pltpu.SemaphoreType.DMA((30,)),
            pltpu.SemaphoreType.DMA((30,)),
            pltpu.SemaphoreType.REGULAR,
        ],
        compiler_params=pltpu.CompilerParams(collective_id=0, has_side_effects=True, vmem_limit_bytes=44 << 20),
        name="exchange",
    )(*(pltpu.with_memory_space_constraint(array, pltpu.HBM) for array in (
        east_class, south_class, cond_table, leakage, pad_mask, load_current)))
    return pl.pallas_call(
        store_kernel,
        out_shape=jax.ShapeDtypeStruct((N, N, width), f32),
        in_specs=[vmem],
        out_specs=pl.BlockSpec(memory_space=pltpu.HBM),
        scratch_shapes=[pltpu.SemaphoreType.DMA((CHUNKS, HALVES))],
        compiler_params=pltpu.CompilerParams(vmem_limit_bytes=8 << 20),
        name="store",
    )(inside)


def solution(mesh):
    block = P("gx", "gy")
    return jax.shard_map(
        body,
        mesh=mesh,
        in_specs=(block, block, P(), block, block, P("gx", "gy", None)),
        out_specs=P("gx", "gy", None),
        check_vma=False,
    )
```

```python
import jax
import jax.numpy as jnp
from jax import lax
from jax.experimental import pallas as pl
from jax.experimental.pallas import tpu as pltpu
from jax.sharding import PartitionSpec as P

MESH = pl.DeviceIdType.MESH
PAD_GAIN = 8.0
SPECTRAL_BOUND = 0.995

N = 64
D = 4
LANE = 128
HALVES = 2
PADC = 8
ROWS = N + 2 * D
COLS = N + 2 * PADC
CHUNKS = 4
CROWS = N // CHUNKS


def polynomial():
    b2 = SPECTRAL_BOUND * SPECTRAL_BOUND
    w1 = 1.0 / (1.0 - b2 / 2.0)
    w2 = 1.0 / (1.0 - b2 * w1 / 4.0)
    w3 = 1.0 / (1.0 - b2 * w2 / 4.0)
    return w3 + (1.0 - w3) * w1, w1 * w2 * w3


ALPHA, BETA = polynomial()


def lookup(classes, table):
    value = jnp.full(classes.shape, table[0], jnp.float32)
    for label in range(1, 8):
        value = jnp.where(classes == label, table[label], value)
    return value


def exchange_kernel(
    east_hbm, south_hbm, table_hbm, leak_hbm, pad_hbm, load_hbm,
    out_ref,
    east_ref, south_ref, leak_ref, pad_ref, table_ref,
    raw, rows_in, cols_in, corner_in, plain, turned, coef, coef_side, cond,
    src, tee, you, vee,
    load_sem, own_sem, input_sem, send_sem, recv_sem, ready_sem,
):
    gx, gy = lax.axis_index("gx"), lax.axis_index("gy")
    nx, ny = lax.axis_size("gx"), lax.axis_size("gy")
    up, down = lax.rem(gx + nx - 1, nx), lax.rem(gx + 1, nx)
    west, east = lax.rem(gy + ny - 1, ny), lax.rem(gy + 1, ny)

    odd = lax.rem(gy, 2)
    near, cross = odd * west + (1 - odd) * east, odd * east + (1 - odd) * west
    early = gy // 2 < cross // 2
    late = jnp.logical_not(early)
    is_odd, is_even = odd == 1, odd == 0

    barrier = pltpu.get_barrier_semaphore()

    def signal(semaphore, devices):
        for device in devices:
            pl.semaphore_signal(semaphore, inc=1, device_id=device, device_id_type=MESH)

    across = [(gx, cross), (up, cross), (down, cross)]
    signal(barrier, [(up, gy), (down, gy), (gx, near), (up, near), (down, near)])

    @pl.when(early)
    def _():
        signal(barrier, across)

    inputs = [
        pltpu.make_async_copy(hbm, ref, input_sem.at[k])
        for k, (hbm, ref) in enumerate((
            (east_hbm, east_ref), (south_hbm, south_ref), (leak_hbm, leak_ref), (pad_hbm, pad_ref), (table_hbm, table_ref),
        ))
    ]
    loads = []
    for q in range(CHUNKS):
        part = pl.ds(q * CROWS, CROWS)
        loads.append(pltpu.make_async_copy(load_hbm.at[part], raw.at[part], load_sem.at[q]))
    owns = [
        pltpu.make_async_copy(load_hbm.at[:, pl.ds(0, D), :], cols_in.at[0, :, pl.ds(D, D), :], own_sem.at[0]),
        pltpu.make_async_copy(load_hbm.at[:, pl.ds(N - D, D), :], cols_in.at[1, :, pl.ds(0, D), :], own_sem.at[1]),
    ]
    for copy in inputs + loads + owns:
        copy.start()
    for copy in inputs:
        copy.wait()

    table = [table_ref[label] for label in range(8)]
    pads = pad_ref[...].astype(jnp.float32)
    fields = [
        lookup(east_ref[...], table),
        lookup(south_ref[...], table),
        leak_ref[...] + PAD_GAIN * pads,
        pads,
    ]
    fill = jnp.zeros((N, LANE - N), jnp.float32)
    for a in range(4):
        plain[a, pl.ds(8, N), :] = jnp.concatenate([fields[a], fill], axis=1)

    def turn(rows):
        return jnp.transpose(rows)[0:N]

    column = lax.broadcasted_iota(jnp.int32, (N, LANE), 0)

    def derive(blocks):
        ea, so, extra, pad = (turn(rows) for rows in blocks)
        diagonal = ea + jnp.where(column == 0, 0.0, pltpu.roll(ea, 1, 0)) + so + pltpu.roll(so, 1, 1) + extra
        inverse = 1.0 / diagonal
        coef[0] = jnp.transpose(jnp.concatenate([ea, so], axis=0))
        coef[1] = jnp.transpose(jnp.concatenate([PAD_GAIN * pad * inverse, inverse], axis=0))
        return ea, so, diagonal, pad

    ones = jnp.ones((8, LANE), jnp.float32)
    tail = jnp.ones((LANE - 8 - N, LANE), jnp.float32)
    derive([jnp.concatenate([ones, jnp.concatenate([field, fill], axis=1), tail], axis=0) for field in fields])

    for copy in loads:
        copy.wait()
    pl.semaphore_wait(barrier, 5 + 3 * late.astype(jnp.int32))

    def remote(k, source, target, device):
        return pltpu.make_async_remote_copy(
            src_ref=source, dst_ref=target, send_sem=send_sem.at[k], recv_sem=recv_sem.at[k],
            device_id=device, device_id_type=MESH,
        )

    low, high = pl.ds(0, D), pl.ds(N - D, D)
    coef_x = [
        remote(0, plain.at[:, pl.ds(8, 8), :], plain.at[:, pl.ds(8 + N, 8), :], (up, gy)),
        remote(1, plain.at[:, pl.ds(N, 8), :], plain.at[:, pl.ds(0, 8), :], (down, gy)),
    ]
    bulk_x = [
        remote(2, raw.at[low], rows_in.at[1], (up, gy)),
        remote(3, raw.at[high], rows_in.at[0], (down, gy)),
    ]
    corners = [[], []]
    for k in range(3):
        size = 4 if k == 2 else 2
        wide = pl.ds(N - size, size), pl.ds(0, size)
        for c, (row, device) in enumerate(((N - 3 + k, down), (2 - k, up))):
            land = k if c == 0 else 2 - k
            corners[0].append(remote(18 + 6 * c + k, raw.at[row, wide[0], :], corner_in.at[2 * c, land, pl.ds(D - size, size), :], (device, east)))
            corners[1].append(remote(21 + 6 * c + k, raw.at[row, wide[1], :], corner_in.at[2 * c + 1, land, pl.ds(0, size), :], (device, west)))
    bulk_y = [[], []]
    for q in range(CHUNKS):
        part = pl.ds(q * CROWS, CROWS)
        bulk_y[0].append(remote(8 + q, raw.at[part, high, :], cols_in.at[0, part, pl.ds(0, D), :], (gx, east)))
        bulk_y[1].append(remote(12 + q, raw.at[part, low, :], cols_in.at[1, part, pl.ds(D, D), :], (gx, west)))
    coef_y = [
        remote(16, turned.at[:, pl.ds(PADC + N - D, D), :], turned.at[:, pl.ds(PADC - D, D), :], (gx, east)),
        remote(17, turned.at[:, pl.ds(PADC, D), :], turned.at[:, pl.ds(PADC + N, D), :], (gx, west)),
    ]

    def send(way, first, last):
        for copy in bulk_y[way][first:last] + (corners[way] if first == 0 else []):
            copy.start()

    @pl.when(late)
    def _():
        signal(ready_sem, across)

    for copy in coef_x + bulk_x:
        copy.start()

    @pl.when(jnp.logical_and(early, is_odd))
    def _():
        send(1, 0, CHUNKS)

    @pl.when(jnp.logical_and(early, is_even))
    def _():
        send(0, 0, CHUNKS)

    @pl.when(jnp.logical_and(late, is_odd))
    def _():
        send(0, 0, CHUNKS)
        send(1, 0, 2)

    @pl.when(jnp.logical_and(late, is_even))
    def _():
        send(1, 0, CHUNKS)
        send(0, 0, 2)

    tiles = [8 + 8 * t for t in range(N // 8)]

    def over_lanes(values):
        return jnp.transpose(jnp.broadcast_to(values, (LANE, LANE)))

    def spread(row, source_of):
        wide = []
        for pair in range(2):
            block = over_lanes(coef[pair, pl.ds(row + D, 1), :])
            wide += [block[0:N], block[N : 2 * N]]
        for a in range(4):
            cond[row, a, pl.ds(PADC, N), :] = wide[a]
        for half in range(HALVES):
            src[row, half, pl.ds(PADC, N), :] = wide[2] - source_of(row, half) * wide[3]

    def spread_side(row):
        block = over_lanes(coef_side[0, pl.ds(row + D, 1), :] + coef_side[1, pl.ds(row + D + ROWS // 2, 1), :])
        for k in range(2):
            for side, e in enumerate((PADC - D, PADC + N - D)):
                for a in range(4):
                    at = k * N + (side * 4 + a) * 8
                    cond[row + k * (ROWS // 2), a, pl.ds(e, 8), :] = block[at : at + 8]

    def step(stage, row, columns):
        for e in columns:
            here, before = pl.ds(e, 8), pl.ds(e - 1, 8)
            ea, we = cond[row, 0, here, :], cond[row, 0, before, :]
            so, no = cond[row, 1, here, :], cond[row - 1, 1, here, :]
            inverse = cond[row, 3, here, :]
            if stage == 3:
                inverse = inverse * BETA
            field = (src, tee, you, vee)[stage - 1]
            for half in range(HALVES):
                total = ea * field[row, half, pl.ds(e + 1, 8), :] + we * field[row, half, before, :]
                total = total + (so * field[row + 1, half, here, :] + no * field[row - 1, half, here, :])
                total = total * inverse
                if stage == 1:
                    tee[row, half, here, :] = src[row, half, here, :] + total
                elif stage == 2:
                    you[row, half, here, :] = total
                elif stage == 3:
                    vee[row, half, here, :] = ALPHA * tee[row, half, here, :] + total
                else:
                    out_ref[row - D, half, here, :] = src[row, half, here, :] + total

    def rows_loop(first, last, unroll, work):
        blocks = (last - first) // unroll

        def body(block, carry):
            for k in range(unroll):
                work(first + D + block * unroll + k)
            return carry

        lax.fori_loop(0, blocks, body, 0)
        for row in range(first + blocks * unroll, last):
            work(row + D)

    def sweep(stage, first, last, columns, unroll=1):
        rows_loop(first, last, unroll, lambda row: step(stage, row, columns))

    def own_load(r, half):
        return raw[r - D, :, pl.ds(half * LANE, LANE)]

    def second_sends(last_only):
        for when, way, begin in (
            (jnp.logical_and(early, is_odd), 0, 0), (jnp.logical_and(early, is_even), 1, 0),
            (jnp.logical_and(late, is_odd), 1, 2), (jnp.logical_and(late, is_even), 0, 2),
        ):
            @pl.when(when)
            def _(way=way, begin=begin):
                send(way, CHUNKS - 1 if last_only else begin, CHUNKS if last_only else CHUNKS - 1)

    def front(first, last):
        def body(block, carry):
            row = first + D + 2 * block
            for k in range(2):
                step(2, row - 6 + k, tiles)
            for k in range(2):
                step(1, row - 3 + k, tiles)
            for k in range(2):
                spread(row + k, own_load)
            return carry

        lax.fori_loop(0, (last - first) // 2, body, 0)

    rows_loop(0, 8, 2, lambda row: spread(row, own_load))
    sweep(1, 1, 5, tiles)
    front(8, N // 2)

    for copy in coef_x:
        copy.wait_recv()
    for a, value in enumerate(derive(
            [jnp.concatenate([plain[a, pl.ds(0, COLS), :], tail[0 : LANE - COLS]], axis=0) for a in range(4)])):
        turned[a, pl.ds(PADC, N), :] = value
    front(N // 2, N)

    @pl.when(early)
    def _():
        pl.semaphore_wait(ready_sem, len(across))

    for copy in coef_y:
        copy.start()
    second_sends(False)
    second_sends(True)

    sweep(1, 61, 63, tiles)
    sweep(2, 58, 62, tiles)
    sweep(3, 3, 61, tiles)
    sweep(4, 4, 60, tiles)

    for copy in bulk_x:
        copy.wait_recv()
    rows_loop(-D, 0, 2, lambda row: spread(
        row, lambda r, half: rows_in[0, r, :, pl.ds(half * LANE, LANE)]))
    rows_loop(0, 1, 1, lambda row: spread(row, own_load))
    rows_loop(N, N + D, 2, lambda row: spread(
        row, lambda r, half: rows_in[1, r - N - D, :, pl.ds(half * LANE, LANE)]))
    for stage in (1, 2, 3, 4):
        sweep(stage, stage - D, 5, tiles)
        sweep(stage, N - D, N + D - stage, tiles)

    for copy in coef_y:
        copy.wait_recv()
    place = lax.broadcasted_iota(jnp.int32, (8, LANE), 0)
    values = []
    for side in range(2):
        ea, so, diagonal, pad = (turned[a, pl.ds(PADC - D + side * N, 8), :] for a in range(4))
        inverse = 1.0 / (diagonal + jnp.where(place == D, pltpu.roll(ea, 1, 0), 0.0))
        values += [ea, so, PAD_GAIN * pad * inverse, inverse]
    values, none = jnp.concatenate(values, axis=0), jnp.zeros((N, LANE), jnp.float32)
    coef_side[0] = jnp.transpose(jnp.concatenate([values, none], axis=0))
    coef_side[1] = jnp.transpose(jnp.concatenate([none, values], axis=0))
    rows_loop(-D, ROWS // 2 - D, 2, spread_side)
    for copy in owns:
        copy.wait()
    first = pl.ds(PADC, D)
    for c, top in enumerate((0, D + N)):
        for k in range(D):
            gain, inverse = cond[top + k, 2, first, :], cond[top + k, 3, first, :]
            for half in range(HALVES):
                load = rows_in[c, k, pl.ds(0, D), pl.ds(half * LANE, LANE)]
                src[top + k, half, first, :] = gain - load * inverse

    def arrived(side, copies):
        for way in range(2):
            @pl.when(side == way)
            def _(way=way):
                for copy in copies[way]:
                    copy.wait_recv()

    def do_side(side):
        halo = PADC - D + side * N
        tile = PADC - D + 1 + side * (N - 1)
        ghost = PADC - D + side * (N + D)
        for q in range(CHUNKS):
            arrived(side, [[bulk_y[way][q]] + (corners[way] if q == 0 else []) for way in range(2)])
            if q == 0:
                for c, first in ((0, 1), (2, D + N)):
                    for k in range(3):
                        for half in range(HALVES):
                            load = corner_in[c + side, k, :, pl.ds(half * LANE, LANE)]
                            gain, inverse = cond[first + k, 2, pl.ds(ghost, D), :], cond[first + k, 3, pl.ds(ghost, D), :]
                            src[first + k, half, pl.ds(ghost, D), :] = gain - load * inverse

            def side_source(row):
                gain, inverse = cond[row, 2, pl.ds(halo, 8), :], cond[row, 3, pl.ds(halo, 8), :]
                for half in range(HALVES):
                    load = cols_in[side, row - D, :, pl.ds(half * LANE, LANE)]
                    src[row, half, pl.ds(halo, 8), :] = gain - load * inverse

            rows_loop(q * CROWS, (q + 1) * CROWS, 8, side_source)
            for stage in (1, 2, 3, 4):
                first = stage - D if q == 0 else q * CROWS - stage
                last = N + D - stage if q == CHUNKS - 1 else (q + 1) * CROWS - stage
                sweep(stage, first, last, (tile,), 8)

    do_side(1 - odd)
    do_side(odd)

    for copy in coef_x + bulk_x + coef_y + corners[0] + corners[1] + bulk_y[0] + bulk_y[1]:
        copy.wait_send()


def store_kernel(field, out_hbm, sem):
    copies = []
    for q in range(CHUNKS):
        for half in range(HALVES):
            part = pl.ds(q * CROWS, CROWS)
            copies.append(pltpu.make_async_copy(
                field.at[part, half, pl.ds(PADC, N), :],
                out_hbm.at[part, :, pl.ds(half * LANE, LANE)],
                sem.at[q, half],
            ))
    for copy in copies:
        copy.start()
    for copy in copies:
        copy.wait()


def body(east_class, south_class, cond_table, leakage, pad_mask, load_current):
    vmem, hbm = pl.BlockSpec(memory_space=pltpu.VMEM), pl.BlockSpec(memory_space=pltpu.HBM)
    f32 = jnp.float32
    width = HALVES * LANE
    field = pltpu.VMEM((ROWS, HALVES, COLS, LANE), f32)
    inside = pl.pallas_call(
        exchange_kernel,
        out_shape=jax.ShapeDtypeStruct((N, HALVES, COLS, LANE), f32),
        in_specs=[hbm] * 6,
        out_specs=vmem,
        scratch_shapes=[
            pltpu.VMEM((N, N), jnp.int32),
            pltpu.VMEM((N, N), jnp.int32),
            pltpu.VMEM((N, N), f32),
            pltpu.VMEM((N, N), jnp.int32),
            pltpu.SMEM((8,), f32),
            pltpu.VMEM((N, N, width), f32),
            pltpu.VMEM((2, D, N, width), f32),
            pltpu.VMEM((2, N, 2 * D, width), f32),
            pltpu.VMEM((4, 3, D, width), f32),
            pltpu.VMEM((4, COLS, LANE), f32),
            pltpu.VMEM((4, COLS, LANE), f32),
            pltpu.VMEM((2, LANE, LANE), f32),
            pltpu.VMEM((2, LANE, LANE), f32),
            pltpu.VMEM((ROWS, 4, COLS, LANE), f32),
            field, field, field, field,
            pltpu.SemaphoreType.DMA((CHUNKS,)),
            pltpu.SemaphoreType.DMA((2,)),
            pltpu.SemaphoreType.DMA((5,)),
            pltpu.SemaphoreType.DMA((30,)),
            pltpu.SemaphoreType.DMA((30,)),
            pltpu.SemaphoreType.REGULAR,
        ],
        compiler_params=pltpu.CompilerParams(collective_id=0, has_side_effects=True, vmem_limit_bytes=44 << 20),
        name="exchange",
    )(*(pltpu.with_memory_space_constraint(array, pltpu.HBM) for array in (
        east_class, south_class, cond_table, leakage, pad_mask, load_current)))
    return pl.pallas_call(
        store_kernel,
        out_shape=jax.ShapeDtypeStruct((N, N, width), f32),
        in_specs=[vmem],
        out_specs=pl.BlockSpec(memory_space=pltpu.HBM),
        scratch_shapes=[pltpu.SemaphoreType.DMA((CHUNKS, HALVES))],
        compiler_params=pltpu.CompilerParams(vmem_limit_bytes=8 << 20),
        name="store",
    )(inside)


def solution(mesh):
    block = P("gx", "gy")
    return jax.shard_map(
        body,
        mesh=mesh,
        in_specs=(block, block, P(), block, block, P("gx", "gy", None)),
        out_specs=P("gx", "gy", None),
        check_vma=False,
    )
```
